32 devices in a mesh: section: 2 (over core), tp: 4 (over y, x), fsdp: 4 (over z).
Axes of the slice: x: 2, y: 2, z: 4, core: 2. Of those that a mesh axis runs over, the one named last changes fastest.
Arguments:
- normed: bfloat16 [2, 256, 4608], P('section', 'tp', 'fsdp'), may hold values from -6 to 6
- cotangent: bfloat16 [2, 256, 4608], P('section', 'tp', 'fsdp'), may hold values from -6 to 6
- w_gate: bfloat16 [2, 4608, 18432], P('section', 'fsdp', 'tp'), may hold values from -0.09375 to 0.09375
- w_up: bfloat16 [2, 4608, 18432], P('section', 'fsdp', 'tp'), may hold values from -0.09375 to 0.09375
- w_down: bfloat16 [2, 4608, 18432], P('section', 'fsdp', 'tp'), may hold values from -0.046875 to 0.046875
Outputs:
- passed: bfloat16 [2, 256, 4608], P('section', 'tp', 'fsdp')
- grad_gate: bfloat16 [2, 4608, 18432], P('section', 'fsdp', 'tp')
- grad_up: bfloat16 [2, 4608, 18432], P('section', 'fsdp', 'tp')
- grad_down: bfloat16 [2, 4608, 18432], P('section', 'fsdp', 'tp')
The draws below stay inside these ranges and needn't reach their ends.
All inputs are finite; a program needn't handle non-finite values.
Results may differ from the reference program's by a relative error of at most 0.012.
Values may be sent and summed in bfloat16 or wider, within the bound.
A program may use at most 192 MiB of HBM per device.

```python
import math
import jax
import jax.numpy as jnp

D = 4608
FF = 18432
TOKENS = 256


def block_scale(rng, shape, cuts, low, top_value):
    def one(axis_at, blocks):
        draws = jax.random.uniform(jax.random.fold_in(jax.random.fold_in(rng, 6), axis_at), (blocks,), jnp.float32, low / len(cuts), top_value / len(cuts))
        return jnp.repeat(jnp.exp(draws), shape[axis_at] // blocks).reshape((-1,) + (1,) * (len(shape) - axis_at - 1))

    level = one(*cuts[0])
    for cut in cuts[1:]:
        level = level * one(*cut)
    return level


def centred(stream_key, shape, width, limit, shards=(), dtype=jnp.bfloat16):
    drawn = width * jax.random.normal(stream_key, shape, jnp.float32)
    if shards:
        drawn = drawn * block_scale(stream_key, shape, shards, -0.22, 0.18)
    return jnp.clip(drawn, -limit, limit).astype(dtype)


def setup_inputs(seed: int = 0) -> dict:
    key_list = jax.random.split(jax.random.key(seed), 6)
    normed = centred(key_list[0], (2, TOKENS, D), 1.0, 6.0, ((0, 2), (1, 4), (2, 4)))
    cotangent = centred(key_list[1], (2, TOKENS, D), 1.0, 6.0, ((0, 2), (1, 4), (2, 4)))
    w_gate = centred(key_list[2], (2, D, FF), D ** -0.5, 0.09375, ((0, 2), (1, 4), (2, 4)))
    w_up = centred(key_list[3], (2, D, FF), D ** -0.5, 0.09375, ((0, 2), (1, 4), (2, 4)))
    w_down = centred(key_list[4], (2, D, FF), FF ** -0.5, 0.046875, ((0, 2), (1, 4), (2, 4)))
    return {"normed": normed, "cotangent": cotangent, "w_gate": w_gate, "w_up": w_up, "w_down": w_down}


def activate(gate, up, back):
    coeff = math.sqrt(2.0 / math.pi)
    inner = jnp.tanh(coeff * (gate + 0.044715 * gate * gate * gate))
    act = 0.5 * gate * (1.0 + inner)
    slope = 0.5 * (1.0 + inner) + 0.5 * gate * (1.0 - inner * inner) * coeff * (1.0 + 3.0 * 0.044715 * gate * gate)
    hidden = (act * up).astype(jnp.bfloat16)
    d_gate = (back * up * slope).astype(jnp.bfloat16)
    d_up = (back * act).astype(jnp.bfloat16)
    return (hidden, d_gate, d_up)

def layer_back(rows, cot, wgate, wup, wdown):
    gate = jnp.dot(rows, wgate, preferred_element_type=jnp.float32)
    up = jnp.dot(rows, wup, preferred_element_type=jnp.float32)
    back = jnp.dot(cot, wdown, preferred_element_type=jnp.float32)
    hidden, d_gate, d_up = activate(gate, up, back)
    scale = 1.0 / math.sqrt(TOKENS)
    g_gate = (jnp.dot(rows.T, d_gate, preferred_element_type=jnp.float32) * scale).astype(jnp.bfloat16)
    g_up = (jnp.dot(rows.T, d_up, preferred_element_type=jnp.float32) * scale).astype(jnp.bfloat16)
    g_down = (jnp.dot(cot.T, hidden, preferred_element_type=jnp.float32) * scale).astype(jnp.bfloat16)
    branch = jnp.dot(d_gate, wgate.T, preferred_element_type=jnp.float32) + jnp.dot(d_up, wup.T, preferred_element_type=jnp.float32)
    handed = (cot.astype(jnp.float32) + branch).astype(jnp.bfloat16)
    return (handed, g_gate, g_up, g_down)

def reference(normed, cotangent, w_gate, w_up, w_down):
    first = layer_back(normed[0], cotangent[0], w_gate[0], w_up[0], w_down[0])
    second = layer_back(normed[1], cotangent[1], w_gate[1], w_up[1], w_down[1])
    passed = jnp.stack([second[0], first[0]])
    grad_gate = jnp.stack([first[1], second[1]])
    grad_up = jnp.stack([first[2], second[2]])
    grad_down = jnp.stack([first[3], second[3]])
    return (passed, grad_gate, grad_up, grad_down)
```

```python
import math

import jax
import jax.numpy as jnp
from jax import lax
from jax.sharding import PartitionSpec as P


def shift(value, axis, steps):
    count = lax.axis_size(axis)
    pairs = [(source, (source + steps) % count) for source in range(count)]
    return lax.ppermute(value, axis, pairs)


def wide(value):
    return value.astype(jnp.float32)


def piece(value, index, rows, start, size):
    return lax.dynamic_slice_in_dim(value, index * rows + start, size, 0)


def chain_sum(part, axis, start, size, steps, direction):
    count = lax.axis_size(axis)
    me = lax.axis_index(axis)
    rows = part.shape[0] // count
    arrived = None
    for far in range(steps, 0, -1):
        mine = piece(part, (me + direction * far + count) % count, rows, start, size)
        if arrived is not None:
            mine = (wide(mine) + wide(arrived)).astype(jnp.bfloat16)
        arrived = shift(mine, axis, direction)
    return arrived


def sum_to_owner(part, axis):
    count = lax.axis_size(axis)
    me = lax.axis_index(axis)
    rows = part.shape[0] // count
    far = count // 2
    near = count - 1 - far
    half = rows // 2
    spans = ((0, half), (half, rows - half))
    terms = []
    for index, (start, size) in enumerate(spans):
        total = wide(piece(part, me, rows, start, size))
        for direction, steps in ((1, far if index == 0 else near), (-1, near if index == 0 else far)):
            if steps:
                total = total + wide(chain_sum(part, axis, start, size, steps, direction))
        terms.append(total)
    return terms


def chain_copy(own, axis, steps, direction):
    out = []
    for _ in range(steps):
        own = shift(own, axis, direction)
        out.append(own)
    return out


def gather_rolled(halves, axis):
    count = lax.axis_size(axis)
    far = count // 2
    near = count - 1 - far
    blocks = []
    for index, own in enumerate(halves):
        up = chain_copy(own, axis, far if index == 0 else near, 1)
        down = chain_copy(own, axis, near if index == 0 else far, -1)
        blocks.append([own] + up + down[::-1])
    return jnp.concatenate([item for pair in zip(*blocks) for item in pair], axis=0)


def roll_blocks(value, axis):
    count = lax.axis_size(axis)
    me = lax.axis_index(axis)
    rows = value.shape[0] // count
    return jnp.concatenate(
        [piece(value, (me - step + count) % count, rows, 0, rows) for step in range(count)], axis=0
    )


def gather_tokens(own, axis):
    return jnp.concatenate(
        [own] + [shift(own, axis, step) for step in range(1, lax.axis_size(axis))], axis=0
    )


def gelu_parts(gate):
    coeff = math.sqrt(2.0 / math.pi)
    inner = jnp.tanh(coeff * (gate + 0.044715 * gate * gate * gate))
    act = 0.5 * gate * (1.0 + inner)
    slope = 0.5 * (1.0 + inner) + 0.5 * gate * (1.0 - inner * inner) * coeff * (
        1.0 + 3.0 * 0.044715 * gate * gate
    )
    return act, slope


def project(left, right):
    return jnp.dot(left, right, preferred_element_type=jnp.float32).astype(jnp.bfloat16)


def column_grad(left, right, scale):
    out = lax.dot_general(
        left, right, (((0,), (0,)), ((), ())), preferred_element_type=jnp.float32
    )
    return (out * scale).astype(jnp.bfloat16)[None]


def row_back(grads, weight):
    return lax.dot_general(
        grads, weight, (((1,), (1,)), ((), ())), preferred_element_type=jnp.float32
    )


def local(normed, cotangent, w_gate, w_up, w_down):
    cot_own = cotangent[0]
    rows_all = gather_tokens(normed[0], "tp")
    cot_all = gather_tokens(cot_own, "tp")
    scale = 1.0 / math.sqrt(rows_all.shape[0])
    gate = sum_to_owner(project(rows_all, w_gate[0]), "fsdp")
    back = sum_to_owner(project(cot_all, w_down[0]), "fsdp")
    up = sum_to_owner(project(rows_all, w_up[0]), "fsdp")
    parts = [gelu_parts(item) for item in gate]
    d_up = [(b * act).astype(jnp.bfloat16) for b, (act, _) in zip(back, parts)]
    d_gate = [(b * u * slope).astype(jnp.bfloat16) for b, u, (_, slope) in zip(back, up, parts)]
    hidden = [(act * u).astype(jnp.bfloat16) for u, (act, _) in zip(up, parts)]
    rows_rolled = roll_blocks(rows_all, "fsdp")
    cot_rolled = roll_blocks(cot_all, "fsdp")
    d_up = gather_rolled(d_up, "fsdp")
    grad_up = column_grad(rows_rolled, d_up, scale)
    d_gate = gather_rolled(d_gate, "fsdp")
    grad_gate = column_grad(rows_rolled, d_gate, scale)
    branch = row_back(d_up, w_up[0]) + row_back(d_gate, w_gate[0])
    hidden = gather_rolled(hidden, "fsdp")
    grad_down = column_grad(cot_rolled, hidden, scale)
    branch = roll_blocks(branch.astype(jnp.bfloat16), "fsdp")
    own = cot_own.shape[0]
    total = wide(cot_own) + wide(branch[:own])
    for step in range(1, lax.axis_size("tp")):
        total = total + wide(shift(branch[step * own : (step + 1) * own], "tp", -step))
    passed = shift(total.astype(jnp.bfloat16), "section", 1)
    return (passed[None], grad_gate, grad_up, grad_down)


def solution(mesh):
    in_specs = (
        P("section", "tp", "fsdp"),
        P("section", "tp", "fsdp"),
        P("section", "fsdp", "tp"),
        P("section", "fsdp", "tp"),
        P("section", "fsdp", "tp"),
    )
    out_specs = (
        P("section", "tp", "fsdp"),
        P("section", "fsdp", "tp"),
        P("section", "fsdp", "tp"),
        P("section", "fsdp", "tp"),
    )
    return jax.shard_map(local, mesh=mesh, in_specs=in_specs, out_specs=out_specs, check_vma=False)
```
